768 devices in a mesh: grp: 48 (over z_lo, x, core), tp: 16 (over z_hi, y).
Axes of the slice: x: 4, y: 8, z: 12 (z_hi: 2, z_lo: 6; z = z_hi * 6 + z_lo), core: 2. Of those that a mesh axis runs over, the one named last changes fastest.
Arguments:
- query: bfloat16 [96, 5120], P('grp'), may hold values from -6 to 6
- key_cache: bfloat16 [96, 2048, 1024], P('grp', 'tp'), may hold values from -6 to 6
- value_cache: bfloat16 [96, 2048, 1024], P('grp', 'tp'), may hold values from -6 to 6
- lengths: int32 [96], P('grp'), may hold values from 128 to 2048
- route: int32 [96], replicated, may hold values from 0 to 95, each once
- out_weight: bfloat16 [5120, 5120], P(None, 'tp'), may hold values from -1.5 to 1.5
Outputs:
- inbox: bfloat16 [96, 5120], P('grp', 'tp')
The draws below stay inside these ranges and needn't reach their ends.
Inputs may be any that keep to these rules, and one draw needn't show every extreme that they name: lengths are at least one block of 128 positions. `route`: every inbox row is named by exactly one trajectory.
All inputs are finite; a program needn't handle non-finite values.
Results may differ from the reference program's by a relative error of at most 0.0095.
Values may be sent and summed in bfloat16 or wider, within the bound.
A program may use at most 32 MiB of HBM per device.

```python
import jax
import jax.numpy as jnp
from jax import lax

D = 5120
HEADS = 40
KV_HEADS = 8
HEAD_DIM = 128
CTX_DEV = 128
CTX = 2048
TRAJS = 96
N_TP = 16


def draw_query(key, part):
    sample = jax.random.truncated_normal(jax.random.fold_in(key, 11), -6.0, 6.0, (TRAJS, D), jnp.float32)
    return sample.astype(jnp.bfloat16)


def draw_key_cache(key, part):
    sample = jax.random.truncated_normal(jax.random.fold_in(key, 12), -6.0, 6.0, (TRAJS, CTX, KV_HEADS * HEAD_DIM), jnp.float32)
    return sample.astype(jnp.bfloat16)


def place_ends(values, own_key, low, top_value):
    longest = values.shape.index(max(values.shape))
    spots = []
    for shift in (0, 1):
        where = [jax.random.randint(jax.random.fold_in(own_key, axis), (), 0, length) for axis, length in enumerate(values.shape)]
        where[longest] = (where[longest] + shift) % values.shape[longest]
        spots.append(tuple(where))
    return values.at[spots[0]].set(low).at[spots[1]].set(top_value)


def block_levels(key, extent, shards, smallest, top_value):
    loudness, own = 1.0, jax.random.fold_in(key, 6)
    for axis_at, blocks in shards:
        steps = jnp.exp(jax.random.uniform(jax.random.fold_in(own, axis_at), (blocks,), jnp.float32, smallest / len(shards), top_value / len(shards)))
        loudness = loudness * jnp.repeat(steps, extent[axis_at] // blocks).reshape([-1 if axis == axis_at else 1 for axis in range(len(extent))])
    return loudness


def noise(rng, shape, deviation, bound, cuts=(), held_as=jnp.bfloat16):
    entries = deviation * jax.random.normal(rng, shape, jnp.float32)
    if cuts:
        entries = entries * block_levels(rng, shape, cuts, -0.22, 0.18)
    return jnp.clip(entries, -bound, bound).astype(held_as)


def setup_inputs(seed: int = 0) -> dict:
    streams_of = jax.random.split(jax.random.key(seed), 7)
    query = draw_query(jax.random.fold_in(streams_of[6], 71), 0)
    key_cache = draw_key_cache(jax.random.fold_in(streams_of[6], 71), 0)
    value_cache = noise(streams_of[2], (TRAJS, CTX, KV_HEADS * HEAD_DIM), 1.0, 6.0, ((0, 48), (1, 16)))
    lengths = place_ends(jax.random.randint(streams_of[3], (TRAJS,), CTX_DEV, CTX + 1), jax.random.fold_in(streams_of[3], 1), CTX_DEV, CTX).astype(jnp.int32)
    route = jax.random.permutation(streams_of[4], TRAJS).astype(jnp.int32)
    out_weight = noise(streams_of[5], (D, D), 16 ** -0.5, 1.5, ((1, 16),))
    return {"query": query, "key_cache": key_cache, "value_cache": value_cache, "lengths": lengths, "route": route, "out_weight": out_weight}


def one_trajectory(args):
    query_row, keys, values, length = args
    group = HEADS // KV_HEADS
    q = query_row.astype(jnp.float32).reshape(KV_HEADS, group, HEAD_DIM)
    k = keys.astype(jnp.float32).reshape(N_TP, CTX_DEV, KV_HEADS, HEAD_DIM)
    v = values.astype(jnp.float32).reshape(N_TP, CTX_DEV, KV_HEADS, HEAD_DIM)
    scores = jnp.einsum('kgd,btkd->bkgt', q, k) / jnp.sqrt(jnp.float32(HEAD_DIM))
    places = jnp.arange(CTX, dtype=jnp.int32).reshape(N_TP, 1, 1, CTX_DEV)
    live = places < length
    scores = jnp.where(live, scores, jnp.float32(-1e+30))
    blockmax = lax.optimization_barrier(jnp.max(scores, axis=3))
    expo = jnp.where(live, jnp.exp(scores - blockmax[..., None]), jnp.float32(0.0))
    blocksum = lax.optimization_barrier(jnp.sum(expo, axis=3))
    weights = expo.astype(jnp.bfloat16).astype(jnp.float32)
    blockout = jnp.einsum('bkgt,btkd->bkgd', weights, v)
    peak = lax.optimization_barrier(jnp.max(blockmax, axis=0))
    factor = jnp.exp(blockmax - peak[None])
    total = lax.optimization_barrier(jnp.sum(factor * blocksum, axis=0))
    combined = lax.optimization_barrier(jnp.sum(factor[..., None] * blockout, axis=0))
    return (combined / total[..., None]).reshape(D).astype(jnp.bfloat16)

def reference(query, key_cache, value_cache, lengths, route, out_weight):
    attended = lax.map(one_trajectory, (query, key_cache, value_cache, lengths))
    projected = jnp.dot(attended, out_weight, preferred_element_type=jnp.float32).astype(jnp.bfloat16)
    inbox = jnp.zeros((TRAJS, D), jnp.bfloat16).at[route].set(projected)
    return inbox
```

```python
import functools

import jax
import jax.numpy as jnp
from jax import lax
from jax.experimental import pallas as pl
from jax.experimental.pallas import tpu as pltpu
from jax.sharding import Mesh
from jax.sharding import PartitionSpec as P

HEADS = 40
KV_HEADS = 8
HEAD_DIM = 128
GROUP = HEADS // KV_HEADS
BLOCK = 128
NZL, NX, NC, NZH, NY = 6, 4, 2, 2, 8
NZ = NZL * NZH
PAD = 8
MESH = pl.DeviceIdType.MESH
F32 = jnp.float32
BF16 = jnp.bfloat16
TINY = 1e-30

Y_STEPS = (4, 3, 5, 2, 6, 1, 7)
Z_STEPS = (6, 5, 7, 4, 8, 3, 9, 2, 10, 1, 11)
X_STEPS = tuple((dx, dc) for dx in (2, 1, 3, 0) for dc in (1, 0) if (dx, dc) != (0, 0))
ARRIVAL = (0, 1, 7, 2, 6, 3, 5, 4)


def split3(row):
    one = row.astype(BF16).astype(F32)
    two = (row - one).astype(BF16).astype(F32)
    return one, two, row - one - two


def with_rows(tile, rows):
    at = lax.broadcasted_iota(jnp.int32, (PAD, 128), 0)
    for k, row in enumerate(rows):
        tile = jnp.where(at == GROUP + k, jnp.broadcast_to(row, (PAD, 128)), tile)
    return tile


def halves(tile):
    wide = tile.astype(F32)
    return wide[:PAD], wide[PAD:]


def kernel(
    q_hbm, k_hbm, v_hbm, w_hbm, len_ref, route_ref, out_ref,
    q_in, k_in, v_in, w_in, q_diag, part, part_got, half, half_got, give, give_got, row, row_got, pick,
    load_sem, ys_sem, yr_sem, zs_sem, zr_sem, xs_sem, xr_sem, gs_sem, gr_sem,
):
    zl, x, c = lax.axis_index("zl"), lax.axis_index("x"), lax.axis_index("c")
    zh, y = lax.axis_index("zh"), lax.axis_index("y")
    z = zh * NZL + zl

    loads = [
        pltpu.make_async_copy(src, dst, load_sem.at[n])
        for n, (src, dst) in enumerate(((q_hbm, q_in), (k_hbm, k_in), (v_hbm, v_in), (w_hbm, w_in)))
    ]
    for load in loads:
        load.start()

    def y_peer(d):
        return {"y": lax.rem(y + d, NY)}

    def z_peer(d):
        to = lax.rem(z + d, NZ)
        return {"zh": to // NZL, "zl": lax.rem(to, NZL)}

    def x_peer(dx, dc):
        return {"x": lax.rem(x + dx, NX), "c": lax.rem(c + dc, NC)}

    peers = [z_peer(d) for d in Z_STEPS] + [y_peer(d) for d in Y_STEPS] + [x_peer(*d) for d in X_STEPS]
    barrier = pltpu.get_barrier_semaphore()
    for peer in peers:
        pl.semaphore_signal(barrier, inc=1, device_id=peer, device_id_type=MESH)

    lane = lax.broadcasted_iota(jnp.int32, (1, NZL * 2 * PAD), 1)
    goes = jnp.zeros((1, NZL * 2 * PAD), jnp.int32)
    for d in range(NZL):
        from_zl = lax.rem(z - d + NZ, NZL)
        for b in range(2):
            to = route_ref[((from_zl * NX + x) * NC + c) * 2 + b]
            goes = jnp.where(lane // PAD == d * 2 + b, to, goes)
    up = lax.broadcasted_iota(jnp.int32, (NX * NC * 2 * PAD, NZL * 2 * PAD), 0)
    across = lax.broadcasted_iota(jnp.int32, (NX * NC * 2 * PAD, NZL * 2 * PAD), 1)
    slot = up // PAD
    slot_x = lax.rem(x + slot // 4, NX)
    slot_c = lax.rem(c + lax.rem(slot // 2, 2), NC)
    slot_row = ((zl * NX + slot_x) * NC + slot_c) * 2 + lax.rem(slot, 2)
    chosen = (slot_row == jnp.broadcast_to(goes, slot_row.shape)) & (lax.rem(up, PAD) == lax.rem(across, PAD))
    pick[...] = jnp.where(chosen, F32(1.0), F32(0.0)).astype(BF16)

    q_diag[...] = jnp.zeros_like(q_diag)
    loads[0].wait()
    q_wide = q_in[...].astype(F32)
    for b in range(2):
        for k in range(KV_HEADS):
            for g in range(GROUP):
                at = (k * GROUP + g) * HEAD_DIM
                to = b * KV_HEADS + k
                q_diag[to * PAD + g : to * PAD + g + 1, to * HEAD_DIM : (to + 1) * HEAD_DIM] = q_wide[
                    b : b + 1, at : at + HEAD_DIM
                ]
    q_all = q_diag[...].astype(BF16)

    loads[1].wait()
    width = KV_HEADS * HEAD_DIM
    contract = (((1,), (1,)), ((), ()))
    scores = lax.dot_general(k_in[0], q_all[:, :width], contract, preferred_element_type=F32)
    scores += lax.dot_general(k_in[1], q_all[:, width:], contract, preferred_element_type=F32)
    scores = scores * F32(HEAD_DIM**-0.5)
    place = (zh * NY + y) * BLOCK + lax.broadcasted_iota(jnp.int32, (BLOCK, 128), 0)
    length = jnp.where(lax.broadcasted_iota(jnp.int32, (BLOCK, 128), 1) < 64, len_ref[0], len_ref[1])
    live = place < length
    scores = jnp.where(live, scores, F32(-1e30))
    shift = jnp.max(scores, axis=0, keepdims=True).astype(BF16).astype(F32)
    expo = jnp.where(live, jnp.exp(scores - shift), F32(0.0))
    total = jnp.sum(expo, axis=0, keepdims=True)
    weights = expo.T.astype(BF16)
    loads[2].wait()
    outs = [jnp.dot(weights[b * 64 : b * 64 + 64], v_in[b], preferred_element_type=F32) for b in range(2)]
    total_hi, total_lo, _ = split3(total)
    for k in range(KV_HEADS):
        tiles = [o[k * PAD : (k + 1) * PAD, k * HEAD_DIM : (k + 1) * HEAD_DIM] for o in outs]
        tiles[0] = with_rows(tiles[0], (shift, total_hi, total_lo))
        part[k] = jnp.concatenate(tiles, axis=0).astype(BF16)

    pl.semaphore_wait(barrier, len(peers))

    sent = []
    for d in Y_STEPS:
        sent.append(
            pltpu.make_async_remote_copy(
                part.at[lax.rem(y + d, NY)], part_got.at[d], ys_sem.at[d], yr_sem.at[d],
                device_id=y_peer(d), device_id_type=MESH,
            )
        )
        sent[-1].start()
    got = {d: s for d, s in zip(Y_STEPS, sent)}
    tiles = []
    for d in ARRIVAL:
        if d:
            got[d].wait_recv()
        tiles.append(halves(part_got[d] if d else part[y]))
    shifts = [t[0][GROUP : GROUP + 1] for t in tiles]
    peak = functools.reduce(jnp.maximum, shifts)
    scale = [jnp.exp(s - peak) for s in shifts]
    total = sum(w * (t[0][GROUP + 1 : GROUP + 2] + t[0][GROUP + 2 : GROUP + 3]) for w, t in zip(scale, tiles))
    total = jnp.maximum(total, F32(TINY))
    down = lax.broadcasted_iota(jnp.int32, (PAD, 128), 0)
    right = lax.broadcasted_iota(jnp.int32, (PAD, 128), 1)
    mine = [right == b * 64 + y * PAD + down for b in range(2)]

    def column(line, b):
        return jnp.sum(jnp.where(mine[b], jnp.broadcast_to(line, (PAD, 128)), F32(0.0)), axis=1, keepdims=True)

    mixed = []
    for b in range(2):
        mixed.append(sum(column(w / total, b) * t[b] for w, t in zip(scale, tiles)))
    mixed[0] = with_rows(mixed[0], split3(peak + jnp.log(total)))
    half[...] = jnp.concatenate(mixed, axis=0).astype(BF16)

    got = {}
    for d in Z_STEPS:
        got[d] = pltpu.make_async_remote_copy(
            half, half_got.at[d], zs_sem.at[d], zr_sem.at[d], device_id=z_peer(d), device_id_type=MESH
        )
        got[d].start()
        sent.append(got[d])
    held = [None] * NZL
    for d in (0, 1, 5, 2, 4, 3):
        ends = []
        for e in (d, d + NZL):
            if e:
                got[e].wait_recv()
            ends.append(halves(half_got[e] if e else half[...]))
        logs = [jnp.sum(t[0][GROUP:], axis=0, keepdims=True) for t in ends]
        top = jnp.maximum(logs[0], logs[1])
        es = [jnp.exp(v - top) for v in logs]
        share = es[0] / (es[0] + es[1])
        both = []
        for b in range(2):
            part0 = column(share, b)
            both.append(part0 * ends[0][b] + (F32(1.0) - part0) * ends[1][b])
        held[d] = jnp.concatenate(both, axis=0).astype(BF16)
    rows = jnp.concatenate(held, axis=0)
    give[...] = jnp.dot(pick[...], rows, preferred_element_type=F32).astype(BF16).reshape(give.shape)

    got = {}
    for dx, dc in X_STEPS:
        n = dx * NC + dc
        got[n] = pltpu.make_async_remote_copy(
            give.at[n], give_got.at[n], xs_sem.at[n], xr_sem.at[n], device_id=x_peer(dx, dc), device_id_type=MESH
        )
        got[n].start()
        sent.append(got[n])
    whole = give[0].astype(F32)
    for n in (1, 2, 3, 6, 7, 4, 5):
        got[n].wait_recv()
        whole += give_got[n].astype(F32)
    row[...] = whole.astype(BF16)

    got = {}
    for d in Y_STEPS:
        got[d] = pltpu.make_async_remote_copy(
            row, row_got.at[d], gs_sem.at[d], gr_sem.at[d], device_id=y_peer(d), device_id_type=MESH
        )
        got[d].start()
        sent.append(got[d])
    loads[3].wait()
    answer = None
    for d in ARRIVAL:
        if d:
            got[d].wait_recv()
        pieces = halves(row_got[d] if d else row[...])
        spread = jnp.concatenate(
            [
                jnp.concatenate([jnp.where(down == g, t, F32(0.0)) for t in pieces], axis=0)
                for g in range(GROUP)
            ],
            axis=1,
        ).astype(BF16)
        first = pl.multiple_of(lax.rem(y - d + NY, NY) * (GROUP * HEAD_DIM), 128)
        some = lax.dot_general(
            w_in[:, pl.ds(first, GROUP * HEAD_DIM)], spread, contract, preferred_element_type=F32
        )
        answer = some if answer is None else answer + some
    answer = answer.T
    out_ref[...] = jnp.concatenate(
        [jnp.sum(answer[i * PAD : (i + 1) * PAD], axis=0, keepdims=True) for i in range(2)], axis=0
    ).astype(BF16)
    for copy in sent:
        copy.wait_send()


def body(query, key_cache, value_cache, lengths, route, out_weight):
    tile = (2 * PAD, HEAD_DIM)
    rows, width = query.shape[0], out_weight.shape[1]
    anywhere = pl.BlockSpec(memory_space=pl.ANY)
    scalars = pl.BlockSpec(memory_space=pltpu.SMEM)
    sems = pltpu.SemaphoreType.DMA
    return pl.pallas_call(
        kernel,
        out_shape=jax.ShapeDtypeStruct((rows, width), BF16),
        in_specs=[anywhere] * 4 + [scalars] * 2,
        out_specs=pl.BlockSpec(memory_space=pltpu.VMEM),
        scratch_shapes=[
            pltpu.VMEM(query.shape, BF16),
            pltpu.VMEM(key_cache.shape, BF16),
            pltpu.VMEM(value_cache.shape, BF16),
            pltpu.VMEM(out_weight.shape[::-1], BF16),
            pltpu.VMEM((128, 2 * KV_HEADS * HEAD_DIM), F32),
            pltpu.VMEM((KV_HEADS, *tile), BF16),
            pltpu.VMEM((NY, *tile), BF16),
            pltpu.VMEM(tile, BF16),
            pltpu.VMEM((NZ, *tile), BF16),
            pltpu.VMEM((NX * NC, *tile), BF16),
            pltpu.VMEM((NX * NC, *tile), BF16),
            pltpu.VMEM(tile, BF16),
            pltpu.VMEM((NY, *tile), BF16),
            pltpu.VMEM((NX * NC * 2 * PAD, NZL * 2 * PAD), BF16),
            sems((4,)),
            sems((NY,)), sems((NY,)),
            sems((NZ,)), sems((NZ,)),
            sems((NX * NC,)), sems((NX * NC,)),
            sems((NY,)), sems((NY,)),
        ],
        compiler_params=pltpu.CompilerParams(collective_id=0, has_side_effects=True),
    )(query, key_cache, value_cache, out_weight.T, lengths, route)


def solution(mesh):
    finer = Mesh(mesh.devices.reshape(NZL, NX, NC, NZH, NY), ("zl", "x", "c", "zh", "y"))
    grp, tp = ("zl", "x", "c"), ("zh", "y")
    return jax.shard_map(
        body,
        mesh=finer,
        in_specs=(
            P(grp, None),
            P(grp, tp, None),
            P(grp, tp, None),
            P(grp),
            P(),
            P(None, tp),
        ),
        out_specs=P(grp, tp),
        check_vma=False,
    )
```
